128 devices in a mesh: grp: 2 (over core), seq: 32 (over y, x_lo, z), tp: 2 (over x_hi).
Axes of the slice: x: 4 (x_hi: 2, x_lo: 2; x = x_hi * 2 + x_lo), y: 4, z: 4, core: 2. Of those that a mesh axis runs over, the one named last changes fastest.
Arguments:
- prompt_states: bfloat16 [2, 16384, 4096], P(None, ('grp', 'seq'), 'tp'), may hold values from -40 to 40
- q_weight: bfloat16 [4096, 16, 128], P(None, 'tp'), may hold values from -0.09375 to 0.09375
- kv_weight: bfloat16 [4096, 2, 4, 128], P(None, None, 'tp'), may hold values from -0.09375 to 0.09375
- lengths: int32 [2], replicated, may hold values from 4096 to 16384, as said below
- sink_positions: int32 [2, 4], replicated, may hold values from 0 to 2047
Outputs:
- attended: bfloat16 [2, 16384, 2048], P(None, ('grp', 'seq'), 'tp')
- kv_cache: bfloat16 [2, 4, 2, 32, 256, 256], P(None, ('tp', 'grp'), None, 'seq')
The draws below stay inside these ranges and needn't reach their ends.
Inputs may be any that keep to these rules, and one draw needn't show every extreme that they name: `lengths`: at least one request has length 16384.
All inputs are finite; a program needn't handle non-finite values.
Results may differ from the reference program's by a relative error of at most 0.0065.
Values may be sent and summed in bfloat16 or wider, within the bound.
A program may use at most 256 MiB of HBM per device.

```python
import math
import jax
import jax.numpy as jnp
from jax import lax

D = 4096
HD = 128
QH = 16
KVH = 4
SINKS = 4
WINDOW = 4096
REQS = 2
LEN = 16384
SLAB = 256
N_GRP = 2
N_SEQ = 32


def draw_prompt_states(key, part):
    scale_key, base_key = jax.random.split(jax.random.fold_in(key, 17), 2)
    scales = jnp.exp(jax.random.uniform(scale_key, (REQS, LEN, 1), jnp.float32, 0.0, math.log(1.1)))
    states = jax.random.normal(base_key, (REQS, LEN, D), jnp.float32) * scales
    return jnp.clip(states, -40.0, 40.0).astype(jnp.bfloat16)


def draw_lengths(key, part):
    length_key, pick_key = jax.random.split(jax.random.fold_in(key, 29), 2)
    drawn = jax.random.randint(length_key, (REQS,), LEN // 4, LEN + 1, jnp.int32)
    chosen = jax.random.randint(pick_key, (), 0, REQS, jnp.int32)
    full_len = jnp.full((REQS,), LEN, jnp.int32)
    return jnp.where(jnp.arange(REQS, dtype=jnp.int32) == chosen, full_len, drawn)


def touch_ends(values, stream_key, smallest, largest):
    spot = [jax.random.randint(jax.random.fold_in(stream_key, axis), (), 0, length) for axis, length in enumerate(values.shape)]
    main_axis = values.shape.index(max(values.shape))
    beside = spot[:main_axis] + [(spot[main_axis] + 1) % values.shape[main_axis]] + spot[main_axis + 1:]
    return values.at[tuple(spot)].set(smallest).at[tuple(beside)].set(largest)


def block_levels(key, shape, cuts, low, top_value):
    def one(axis_at, blocks):
        heights = jax.random.uniform(jax.random.fold_in(jax.random.fold_in(key, 6), axis_at), (blocks,), jnp.float32, low / len(cuts), top_value / len(cuts))
        return jnp.repeat(jnp.exp(heights), shape[axis_at] // blocks).reshape((-1,) + (1,) * (len(shape) - axis_at - 1))

    level = one(*cuts[0])
    for cut in cuts[1:]:
        level = level * one(*cut)
    return level


def bell_draw(key, extent, width, most, shards=(), kind=jnp.bfloat16):
    loudness = block_levels(key, extent, shards, -0.22, 0.18) if shards else 1.0
    entries = jax.random.normal(key, extent, jnp.float32) * width * loudness
    return jnp.minimum(jnp.maximum(entries, -most), most).astype(kind)


def setup_inputs(seed: int = 0) -> dict:
    keys = jax.random.split(jax.random.key(seed), 6)
    prompt_states = draw_prompt_states(jax.random.fold_in(keys[5], 71), 0)
    q_weight = bell_draw(keys[1], (D, QH, HD), D ** -0.5, 0.09375, ((1, 2),))
    kv_weight = bell_draw(keys[2], (D, 2, KVH, HD), D ** -0.5, 0.09375, ((2, 2),))
    lengths = draw_lengths(jax.random.fold_in(keys[5], 71), 0)
    sink_positions = touch_ends(jax.random.randint(keys[4], (REQS, SINKS), 0, LEN // 8), jax.random.fold_in(keys[4], 1), 0, (LEN // 8) - 1).astype(jnp.int32)
    return dict(prompt_states=prompt_states, q_weight=q_weight, kv_weight=kv_weight, lengths=lengths, sink_positions=sink_positions)


ROPE_BASE = 10000.0
NEG_FILL = -1e+30

def rotate(vectors, positions):
    head_dim = vectors.shape[-1]
    half_dim = head_dim // 2
    ladder = jnp.arange(half_dim, dtype=jnp.float32) * (2.0 / head_dim)
    inv_freq = jnp.exp(-math.log(ROPE_BASE) * ladder)
    angles = positions.astype(jnp.float32)[:, None] * inv_freq[None, :]
    cosine = jnp.cos(angles)[None, :, None, :]
    sine_part = jnp.sin(angles)[None, :, None, :]
    lead_half = vectors[..., :half_dim]
    tail_half = vectors[..., half_dim:]
    return jnp.concatenate([lead_half * cosine - tail_half * sine_part, tail_half * cosine + lead_half * sine_part], axis=-1)

def reference(prompt_states, q_weight, kv_weight, lengths, sink_positions):
    num_reqs, length, model_width = prompt_states.shape
    num_heads, head_dim = (q_weight.shape[1], q_weight.shape[2])
    kv_heads = kv_weight.shape[2]
    share_count = num_heads // kv_heads
    flattened = prompt_states.reshape(num_reqs * length, model_width)
    query_raw = jnp.dot(flattened, q_weight.reshape(model_width, num_heads * head_dim), preferred_element_type=jnp.float32)
    kv_raw = jnp.dot(flattened, kv_weight.reshape(model_width, 2 * kv_heads * head_dim), preferred_element_type=jnp.float32)
    positions = jnp.arange(length, dtype=jnp.int32)
    queries = rotate(query_raw.reshape(num_reqs, length, num_heads, head_dim), positions).astype(jnp.bfloat16)
    kv_raw = kv_raw.reshape(num_reqs, length, 2, kv_heads, head_dim)
    key_rows = rotate(kv_raw[:, :, 0], positions).astype(jnp.bfloat16)
    values = kv_raw[:, :, 1].astype(jnp.bfloat16)
    inv_root = 1.0 / math.sqrt(head_dim)
    block_rows = 512 if length % 512 == 0 else length

    def one_request(packed):
        req_query, req_keys, req_values, prompt_len, sink_pos = packed
        sink_flag = jnp.any(positions[:, None] == sink_pos[None, :], axis=1)
        keys_wide = req_keys.astype(jnp.float32)
        values_wide = req_values.astype(jnp.float32)

        def one_block(block_index):
            start = block_index * block_rows
            query_pos = start + jnp.arange(block_rows, dtype=jnp.int32)
            block_query = lax.dynamic_slice_in_dim(req_query, start, block_rows, 0)
            distance = query_pos[:, None] - positions[None, :]
            visible = (distance >= 0) & (positions[None, :] < prompt_len) & ((distance < WINDOW) | sink_flag[None, :])
            query_wide = block_query.astype(jnp.float32).reshape(block_rows, kv_heads, share_count, head_dim)
            scores = jnp.einsum('qhgd,khd->hgqk', query_wide, keys_wide, precision=lax.Precision.HIGHEST) * inv_root
            scores = jnp.where(visible[None, None], scores, NEG_FILL)
            row_max = lax.optimization_barrier(jnp.max(scores, axis=-1, keepdims=True))
            weights = jnp.where(visible[None, None], jnp.exp(scores - row_max), 0.0)
            sums_now = lax.optimization_barrier(jnp.sum(weights, axis=-1))
            weight_rows = lax.optimization_barrier(weights.astype(jnp.bfloat16)).astype(jnp.float32)
            mixed = jnp.einsum('hgqk,khd->hgqd', weight_rows, values_wide, precision=lax.Precision.HIGHEST)
            mixed = mixed / sums_now[..., None]
            mixed = jnp.transpose(mixed, (2, 0, 1, 3)).reshape(block_rows, num_heads * head_dim)
            live_rows = query_pos < prompt_len
            return jnp.where(live_rows[:, None], mixed, 0.0).astype(jnp.bfloat16)
        blocks = lax.map(one_block, jnp.arange(length // block_rows, dtype=jnp.int32))
        return blocks.reshape(length, num_heads * head_dim)
    attended = lax.map(one_request, (queries, key_rows, values, lengths, sink_positions))
    live_rows = positions[None, :] < lengths[:, None]
    kv_cache = jnp.concatenate([key_rows, values], axis=-1)
    kv_cache = jnp.where(live_rows[:, :, None, None], kv_cache, jnp.zeros_like(kv_cache))
    kv_cache = jnp.transpose(kv_cache, (0, 2, 1, 3))
    kv_cache = kv_cache.reshape(num_reqs, kv_heads, N_GRP, N_SEQ, SLAB, 2 * head_dim)
    return (attended, kv_cache)
```

```python
import math

import jax
import jax.numpy as jnp
from jax import lax
from jax.experimental import pallas as pl
from jax.experimental.pallas import tpu as pltpu
from jax.sharding import PartitionSpec as P

WINDOW = 4096
ROPE_BASE = 10000.0
NEG_FILL = -1e30
FAR = 1 << 30
MESH = pl.DeviceIdType.MESH
CHUNKS = 4
VMEM_BYTES = 60 * 2**20


def place():
    core, seq, tp = lax.axis_index("grp"), lax.axis_index("seq"), lax.axis_index("tp")
    return core, seq // 8, lax.rem(seq // 4, 2), lax.rem(seq, 4), tp


def at(core, y, x, z, tp):
    return (core, y * 8 + x * 4 + z, tp)


def next_row(core, y):
    wraps = (y + 1) // 4
    return lax.rem(core + wraps, 2), lax.rem(y + 1, 4)


def previous_row(core, y):
    wraps = (4 - y) // 4
    return lax.rem(core + wraps, 2), lax.rem(y + 3, 4)


def remote(src, dst, send_sem, recv_sem, target):
    return pltpu.make_async_remote_copy(
        src_ref=src,
        dst_ref=dst,
        send_sem=send_sem,
        recv_sem=recv_sem,
        device_id=target,
        device_id_type=MESH,
    )


def turned(block, cosine, sine):
    return block * cosine + pltpu.roll(block, 64, 1) * sine


def gather_kernel(
    lens, x_hbm, wq_hbm, wkv_hbm, cos_ref, sin_ref, hot_ref,
    q_out, kv_out, sink_out, cache_out,
    x_own, x_far, wq, wkv, acc_q, acc_kv, q_stage, kv_stage, cache_stage, group_kv, sink_stage,
    x_send, x_recv, load_sem, kv_send, kv_recv, kv_keep, q_send, q_recv, q_keep,
    a_send, a_recv, b_send, b_recv, aa_send, aa_recv, bb_send, bb_recv,
    c_send, c_recv, c_keep, s_send, s_recv, s_keep,
):
    core, y, x, z, tp = place()
    up, down = next_row(core, y), previous_row(core, y)
    ahead, behind = at(*up, x, z, tp), at(*down, x, z, tp)
    partner = at(core, y, x, z, 1 - tp)
    twin = at(1 - core, y, x, z, tp)
    side_core = core * (1 - x) + up[0] * x
    side_y = y * (1 - x) + up[1] * x
    side = at(side_core, side_y, 1 - x, z, tp)
    feed_core = core * x + down[0] * (1 - x)
    feed_y = y * x + down[1] * (1 - x)
    feed = at(feed_core, feed_y, 1 - x, z, tp)
    first_row = (core + y) == 0
    row = core * 4 + y
    peers = [at(core, y, x, lax.rem(z + d, 4), tp) for d in (1, 2, 3)]

    barrier = pltpu.get_barrier_semaphore()
    for other in [partner, twin, ahead, behind, side, feed, *peers]:
        pl.semaphore_signal(barrier, inc=1, device_id=other, device_id_type=MESH)

    def sink_target(n):
        slot = lax.rem(row * 2 + x + n, 16)
        return at(slot // 8, lax.rem(slot // 2, 4), lax.rem(slot, 2), z, tp)

    @pl.when(first_row)
    def _():
        for n in range(1, 16):
            pl.semaphore_signal(barrier, inc=1, device_id=sink_target(n), device_id_type=MESH)
        pl.semaphore_wait(barrier, 24)

    @pl.when(jnp.logical_not(first_row))
    def _():
        for x_home in (0, 1):
            pl.semaphore_signal(
                barrier, inc=1, device_id=at(0, 0, x_home, z, tp), device_id_type=MESH
            )
        pl.semaphore_wait(barrier, 11)

    size = 256 // CHUNKS
    spans = [pl.ds(c * size, size) for c in range(CHUNKS)]
    x_copies = [
        remote(x_hbm.at[:, s], x_far.at[:, s], x_send.at[c], x_recv.at[c], partner)
        for c, s in enumerate(spans)
    ]
    for copy in x_copies:
        copy.start()
    loads = [
        pltpu.make_async_copy(x_hbm, x_own, load_sem.at[0]),
        pltpu.make_async_copy(wkv_hbm, wkv, load_sem.at[1]),
        pltpu.make_async_copy(wq_hbm, wq, load_sem.at[2]),
    ]
    for copy in loads:
        copy.start()
    for copy in loads:
        copy.wait()
    own_rows = pl.ds(pl.multiple_of(tp * 2048, 2048), 2048)
    far_rows = pl.ds(pl.multiple_of((1 - tp) * 2048, 2048), 2048)

    def columns(n):
        return pl.ds(pl.multiple_of(n * 256, 256), 256)

    @pl.loop(0, 2)
    def _(n):
        acc_kv[:, :, columns(n)] = jnp.dot(
            x_own[...].reshape(512, 2048),
            wkv[own_rows, columns(n)],
            preferred_element_type=jnp.float32,
        ).reshape(2, 256, 256)

    @pl.loop(0, 4)
    def _(n):
        acc_q[:, :, columns(n)] = jnp.dot(
            x_own[...].reshape(512, 2048),
            wq[own_rows, columns(n)],
            preferred_element_type=jnp.float32,
        ).reshape(2, 256, 256)

    slab_start = (core * 32 + y * 8 + x * 4 + z) * 256
    pending = []
    kv_copies, q_copies, keeps, a_copies, b_copies, aa_copies, bb_copies = [], [], [], [], [], [], []

    def pass_on(c):
        s = spans[c]
        a_copies[c].wait_recv()
        aa = remote(
            kv_out.at[8:12, s], kv_out.at[0:4, s], aa_send.at[c], aa_recv.at[c], ahead
        )
        aa.start()
        aa_copies.append(aa)
        b_copies[c].wait_recv()
        bb = remote(
            kv_out.at[12:16, s], kv_out.at[4:8, s], bb_send.at[c], bb_recv.at[c], ahead
        )
        bb.start()
        bb_copies.append(bb)

    for c in range(CHUNKS):
        s = spans[c]
        x_copies[c].wait_recv()
        cosine, sine = cos_ref[s, :], sin_ref[s, :]

        @pl.loop(0, 2)
        def _(n):
            total = jnp.dot(
                x_far[:, s].reshape(2 * size, 2048),
                wkv[far_rows, columns(n)],
                preferred_element_type=jnp.float32,
            )
            for r in range(2):
                block = total[r * size:(r + 1) * size] + acc_kv[r, s, columns(n)]
                keys = turned(block[:, :128], cosine, sine).astype(jnp.bfloat16)
                both = jnp.concatenate([keys, block[:, 128:].astype(jnp.bfloat16)], axis=1)
                kv_stage[r * 2 + n, s, :] = both
                position = (
                    slab_start + c * size + lax.broadcasted_iota(jnp.int32, (size, 256), 0)
                )
                cache_stage[r, n, s, :] = jnp.where(
                    position < lens[r], both.astype(jnp.float32), 0.0
                ).astype(jnp.bfloat16)

        for d in (1, 2, 3):
            target = lax.rem(z + d, 4)
            copy = remote(
                kv_stage.at[target, s], kv_out.at[16 + z, s],
                kv_send.at[c, d - 1], kv_recv.at[c, d - 1], peers[d - 1],
            )
            copy.start()
            kv_copies.append(copy)
        keep = pltpu.make_async_copy(kv_stage.at[z, s], kv_out.at[16 + z, s], kv_keep.at[c])
        keep.start()

        @pl.loop(0, 4)
        def _(n):
            total = jnp.dot(
                x_far[:, s].reshape(2 * size, 2048),
                wq[far_rows, columns(n)],
                preferred_element_type=jnp.float32,
            )
            for r in range(2):
                block = total[r * size:(r + 1) * size] + acc_q[r, s, columns(n)]
                for k in range(2):
                    head = turned(block[:, k * 128:(k + 1) * 128], cosine, sine)
                    q_stage[r * 2 + n // 2, lax.rem(n, 2) * 2 + k, s, :] = head.astype(
                        jnp.bfloat16
                    )

        for d in (1, 2, 3):
            target = lax.rem(z + d, 4)
            copy = remote(
                q_stage.at[target, :, s], q_out.at[z, :, s],
                q_send.at[c, d - 1], q_recv.at[c, d - 1], peers[d - 1],
            )
            copy.start()
            q_copies.append(copy)
        q_own = pltpu.make_async_copy(q_stage.at[z, :, s], q_out.at[z, :, s], q_keep.at[c])
        q_own.start()
        keeps.append(q_own)

        keep.wait()
        for d in range(3):
            kv_copies[c * 3 + d].wait_recv()
        a = remote(kv_out.at[16:20, s], kv_out.at[8:12, s], a_send.at[c], a_recv.at[c], ahead)
        b = remote(kv_out.at[16:20, s], kv_out.at[12:16, s], b_send.at[c], b_recv.at[c], side)
        a.start()
        b.start()
        a_copies.append(a)
        b_copies.append(b)
        if c >= 1:
            pass_on(c - 1)

    cache_copy = remote(
        cache_stage.at[:, 1 - core], cache_out.at[:, core], c_send.at[0], c_recv.at[0], twin
    )
    cache_copy.start()
    cache_keep = pltpu.make_async_copy(
        cache_stage.at[:, core], cache_out.at[:, core], c_keep.at[0]
    )
    cache_keep.start()

    sink_sends = [
        remote(
            sink_stage, sink_out.at[x], s_send.at[n - 1], s_recv.at[x], sink_target(n)
        )
        for n in range(1, 16)
    ]
    sink_keep = pltpu.make_async_copy(sink_stage, sink_out.at[x], s_keep.at[0])

    @pl.when(first_row)
    def _():
        load = pltpu.make_async_copy(kv_out.at[16:20], group_kv, load_sem.at[0])
        load.start()
        load.wait()
        sink_stage[...] = jnp.dot(
            hot_ref[...], group_kv[...].reshape(1024, 256), preferred_element_type=jnp.float32
        ).astype(jnp.bfloat16)
        for copy in sink_sends:
            copy.start()
        sink_keep.start()

    pass_on(CHUNKS - 1)

    @pl.when(first_row)
    def _():
        sink_keep.wait()
        for copy in sink_sends:
            copy.wait_send()
        remote(sink_stage, sink_out.at[1 - x], s_send.at[0], s_recv.at[1 - x], partner).wait_recv()

    @pl.when(jnp.logical_not(first_row))
    def _():
        for home in (0, 1):
            remote(
                sink_stage, sink_out.at[home], s_send.at[0], s_recv.at[home], partner
            ).wait_recv()

    for copy in keeps:
        copy.wait()
    cache_keep.wait()
    cache_copy.wait()
    for copy in aa_copies + bb_copies:
        copy.wait()
    for copy in q_copies:
        copy.wait()
    for copy in kv_copies + a_copies + b_copies + x_copies:
        copy.wait_send()


SCALE = math.log2(math.e) / math.sqrt(128.0)


def attend_kernel(
    lens, sink_pos, q_ref, kv_ref, sink_ref, out_ref,
    values, peak, total, stage, send_sem, recv_sem, keep_sem,
):
    core, y, x, z, tp = place()
    group = (core * 4 + y) * 2 + x
    peers = [at(core, y, x, lax.rem(z + d, 4), tp) for d in (1, 2, 3)]
    barrier = pltpu.get_barrier_semaphore()
    for other in peers:
        pl.semaphore_signal(barrier, inc=1, device_id=other, device_id_type=MESH)
    pl.semaphore_wait(barrier, 3)

    values[:, :, :128] = kv_ref[:, :, 128:]
    values[:, :, 128:] = jnp.ones((20, 256, 128), jnp.bfloat16)
    request = z // 2
    length = lens[request]
    sink_kv = (sink_ref[0].astype(jnp.float32) + sink_ref[1].astype(jnp.float32)).astype(
        jnp.bfloat16
    )
    pad = jnp.zeros((112, 128), jnp.bfloat16)
    sink_keys = jnp.concatenate([sink_kv[:, :128], pad], axis=0)
    sink_values = jnp.concatenate(
        [
            jnp.concatenate([sink_kv[:, 128:], pad], axis=0),
            jnp.ones((128, 128), jnp.bfloat16),
        ],
        axis=1,
    )

    def fold(queries, keys, vals, visible):
        scores = lax.dot_general(
            queries, keys, (((1,), (1,)), ((), ())), preferred_element_type=jnp.float32
        )
        if visible is not None:
            width = scores.shape[1]
            scores = jnp.where(
                visible[None], scores.reshape(4, 256, width), NEG_FILL
            ).reshape(1024, width)
        old = peak[...]
        new = jnp.maximum(old, jnp.max(scores, axis=1, keepdims=True))
        peak[...] = new
        shift = new[:, :1] * SCALE
        weights = jnp.exp2(scores * SCALE - shift).astype(jnp.bfloat16)
        factor = jnp.exp2((old - new) * SCALE)
        gained = jnp.dot(weights, vals, preferred_element_type=jnp.float32)
        total[...] = total[...] * jnp.concatenate([factor, factor], axis=1) + gained

    def block_mask(first_query, first_key):
        query = first_query + lax.broadcasted_iota(jnp.int32, (256, 256), 0)
        key = first_key + lax.broadcasted_iota(jnp.int32, (256, 256), 1)
        return (query - key >= 0) & (query - key < WINDOW)

    for turn in range(4):
        j = lax.rem(z + 1 + turn, 4)
        queries = q_ref[j].reshape(1024, 128)
        peak[...] = jnp.full((1024, 128), NEG_FILL, jnp.float32)
        total[...] = jnp.zeros((1024, 256), jnp.float32)
        first_query = (16 + j) * 256
        edge_count = jnp.where(group >= 4, 5, j + 1)

        def edge(t, carry):
            slab = jnp.where(t <= j, 16 + j - t, t - 1)
            fold(
                queries, kv_ref[slab, :, :128], values[slab],
                block_mask(first_query, slab * 256),
            )
            return carry

        lax.fori_loop(0, edge_count, edge, 0)

        def middle(k, carry):
            first = 12 - 4 * k
            fold(
                queries,
                kv_ref[pl.ds(first, 4), :, :128].reshape(1024, 128),
                values[pl.ds(first, 4)].reshape(1024, 256),
                None,
            )
            return carry

        lax.fori_loop(0, jnp.minimum(group, 3), middle, 0)
        true_first = (group * 4 + j) * 256
        query_pos = true_first + lax.broadcasted_iota(jnp.int32, (256, 128), 0)
        fold(queries, sink_keys, sink_values, query_pos - sink_pos[...] >= WINDOW)
        mixed = total[:, :128] / total[:, 128:]
        for h in range(4):
            part = mixed[h * 256:(h + 1) * 256]
            stage[turn, :, h * 128:(h + 1) * 128] = jnp.where(
                query_pos < length, part, 0.0
            ).astype(jnp.bfloat16)
        home = out_ref.at[
            request, :, pl.ds(pl.multiple_of(lax.rem(z, 2) * 512, 512), 512)
        ]
        if turn < 3:
            remote(
                stage.at[turn], home, send_sem.at[turn], recv_sem.at[turn], peers[turn]
            ).start()
        else:
            keep = pltpu.make_async_copy(stage.at[3], home, keep_sem.at[0])
            keep.start()
    keep.wait()
    for turn in range(3):
        source = lax.rem(z + 3 - turn, 4)
        landed = out_ref.at[
            source // 2, :, pl.ds(pl.multiple_of(lax.rem(source, 2) * 512, 512), 512)
        ]
        remote(
            stage.at[turn], landed, send_sem.at[turn], recv_sem.at[turn], peers[turn]
        ).wait()


def dma(*shape):
    return pltpu.SemaphoreType.DMA(shape)


def per_device(prompt_states, q_weight, kv_weight, lengths, sink_positions):
    bf16 = jnp.bfloat16
    core, y, x, z, tp = place()
    group = (core * 4 + y) * 2 + x
    wq = q_weight.reshape(4096, 1024)
    wkv = jnp.transpose(kv_weight, (0, 2, 1, 3)).reshape(4096, 512)
    positions = (group * 4 + z) * 256 + jnp.arange(256, dtype=jnp.int32)
    ladder = jnp.arange(64, dtype=jnp.float32) * (2.0 / 128)
    inv_freq = jnp.exp(-math.log(ROPE_BASE) * ladder)
    angles = positions.astype(jnp.float32)[:, None] * inv_freq[None, :]
    cosine, sine = jnp.cos(angles), jnp.sin(angles)
    cos_table = jnp.concatenate([cosine, cosine], axis=1)
    sin_table = jnp.concatenate([-sine, sine], axis=1)
    sinks = jnp.where(z < 2, sink_positions[0], sink_positions[1])
    group_pos = group * 1024 + jnp.arange(1024, dtype=jnp.int32)
    hot = (sinks[:, None] == group_pos[None, :]).astype(bf16)
    hot = jnp.pad(hot, ((0, 12), (0, 0)))
    earlier = jnp.arange(4)[None, :] < jnp.arange(4)[:, None]
    repeated = jnp.any((sinks[:, None] == sinks[None, :]) & earlier, axis=1)
    sink_row = jnp.pad(jnp.where(repeated, FAR, sinks), (0, 124), constant_values=FAR)[None]

    anyspace = pl.BlockSpec(memory_space=pl.ANY)
    vmem = pl.BlockSpec(memory_space=pltpu.VMEM)
    smem = pl.BlockSpec(memory_space=pltpu.SMEM)
    shape = jax.ShapeDtypeStruct
    q_all, kv_all, sink_kv, cache = pl.pallas_call(
        gather_kernel,
        out_shape=(
            shape((4, 4, 256, 128), bf16),
            shape((20, 256, 256), bf16),
            shape((2, 16, 256), bf16),
            shape((2, 2, 256, 256), bf16),
        ),
        in_specs=[smem, anyspace, anyspace, anyspace, vmem, vmem, vmem],
        out_specs=(anyspace, anyspace, anyspace, anyspace),
        scratch_shapes=[
            pltpu.VMEM((2, 256, 2048), bf16),
            pltpu.VMEM((2, 256, 2048), bf16),
            pltpu.VMEM((4096, 1024), bf16),
            pltpu.VMEM((4096, 512), bf16),
            pltpu.VMEM((2, 256, 1024), jnp.float32),
            pltpu.VMEM((2, 256, 512), jnp.float32),
            pltpu.VMEM((4, 4, 256, 128), bf16),
            pltpu.VMEM((4, 256, 256), bf16),
            pltpu.VMEM((2, 2, 256, 256), bf16),
            pltpu.VMEM((4, 256, 256), bf16),
            pltpu.VMEM((16, 256), bf16),
            dma(CHUNKS), dma(CHUNKS), dma(3),
            dma(CHUNKS, 3), dma(CHUNKS, 3), dma(CHUNKS),
            dma(CHUNKS, 3), dma(CHUNKS, 3), dma(CHUNKS),
            dma(CHUNKS), dma(CHUNKS), dma(CHUNKS), dma(CHUNKS),
            dma(CHUNKS), dma(CHUNKS), dma(CHUNKS), dma(CHUNKS),
            dma(1), dma(1), dma(1), dma(15), dma(2), dma(1),
        ],
        compiler_params=pltpu.CompilerParams(
            collective_id=0, has_side_effects=True, vmem_limit_bytes=VMEM_BYTES
        ),
    )(lengths, prompt_states, wq, wkv, cos_table, sin_table, hot)
    attended = pl.pallas_call(
        attend_kernel,
        out_shape=shape((2, 256, 1024), bf16),
        in_specs=[smem, vmem, vmem, vmem, vmem],
        out_specs=anyspace,
        scratch_shapes=[
            pltpu.VMEM((20, 256, 256), bf16),
            pltpu.VMEM((1024, 128), jnp.float32),
            pltpu.VMEM((1024, 256), jnp.float32),
            pltpu.VMEM((4, 256, 512), bf16),
            dma(3), dma(3), dma(1),
        ],
        compiler_params=pltpu.CompilerParams(
            collective_id=1, has_side_effects=True, vmem_limit_bytes=VMEM_BYTES
        ),
    )(lengths, sink_row, q_all, kv_all, sink_kv)
    return attended, cache.reshape(2, 1, 2, 1, 256, 256)


def solution(mesh):
    placed = (
        P(None, ("grp", "seq"), "tp"),
        P(None, "tp", None),
        P(None, None, "tp", None),
        P(),
        P(),
    )
    return jax.shard_map(
        per_device,
        mesh=mesh,
        in_specs=placed,
        out_specs=(P(None, ("grp", "seq"), "tp"), P(None, ("tp", "grp"), None, "seq", None, None)),
        check_vma=False,
    )
```

```python
import math

import jax
import jax.numpy as jnp
from jax import lax
from jax.experimental import pallas as pl
from jax.experimental.pallas import tpu as pltpu
from jax.sharding import PartitionSpec as P

WINDOW = 4096
ROPE_BASE = 10000.0
NEG_FILL = -1e30
FAR = 1 << 30
MESH = pl.DeviceIdType.MESH
CHUNKS = 4
VMEM_BYTES = 60 * 2**20


def place():
    core, seq, tp = lax.axis_index("grp"), lax.axis_index("seq"), lax.axis_index("tp")
    return core, seq // 8, lax.rem(seq // 4, 2), lax.rem(seq, 4), tp


def at(core, y, x, z, tp):
    return (core, y * 8 + x * 4 + z, tp)


def next_row(core, y):
    wraps = (y + 1) // 4
    return lax.rem(core + wraps, 2), lax.rem(y + 1, 4)


def previous_row(core, y):
    wraps = (4 - y) // 4
    return lax.rem(core + wraps, 2), lax.rem(y + 3, 4)


def remote(src, dst, send_sem, recv_sem, target):
    return pltpu.make_async_remote_copy(
        src_ref=src,
        dst_ref=dst,
        send_sem=send_sem,
        recv_sem=recv_sem,
        device_id=target,
        device_id_type=MESH,
    )


def turned(block, cosine, sine):
    return block * cosine + pltpu.roll(block, 64, 1) * sine


SCALE = math.log2(math.e) / math.sqrt(128.0)


def layer_kernel(
    lens, x_hbm, wq_hbm, wkv_hbm, cos_ref, sin_ref, hot_ref, sink_pos,
    out_ref, cache_out,
    x_own, x_far, wq_raw, wkv_raw, spread, wq, wkv, acc_q, acc_kv, q_stage, kv_stage, cache_stage,
    q_all, kv_all, sink_all, sink_stage, values, sink_values, peak, total, scores, stage,
    x_send, x_recv, load_sem, kv_send, kv_recv, kv_keep, q_send, q_recv, q_keep,
    a_send, a_recv, b_send, b_recv, aa_send, aa_recv, bb_send, bb_recv,
    c_send, c_recv, c_keep, s_send, s_recv, s_keep, o_send, o_recv, o_keep,
):
    core, y, x, z, tp = place()
    up, down = next_row(core, y), previous_row(core, y)
    ahead, behind = at(*up, x, z, tp), at(*down, x, z, tp)
    partner = at(core, y, x, z, 1 - tp)
    twin = at(1 - core, y, x, z, tp)
    side_core = core * (1 - x) + up[0] * x
    side_y = y * (1 - x) + up[1] * x
    side = at(side_core, side_y, 1 - x, z, tp)
    feed_core = core * x + down[0] * (1 - x)
    feed_y = y * x + down[1] * (1 - x)
    feed = at(feed_core, feed_y, 1 - x, z, tp)
    first_row = (core + y) == 0
    row = core * 4 + y
    peers = [at(core, y, x, lax.rem(z + d, 4), tp) for d in (1, 2, 3)]

    barrier = pltpu.get_barrier_semaphore()
    for other in [partner, twin, ahead, behind, side, feed, *peers]:
        pl.semaphore_signal(barrier, inc=1, device_id=other, device_id_type=MESH)

    def sink_target(n):
        slot = lax.rem(row * 2 + x + n, 16)
        return at(slot // 8, lax.rem(slot // 2, 4), lax.rem(slot, 2), z, tp)

    @pl.when(first_row)
    def _():
        for n in range(1, 16):
            pl.semaphore_signal(barrier, inc=1, device_id=sink_target(n), device_id_type=MESH)
        pl.semaphore_wait(barrier, 24)

    @pl.when(jnp.logical_not(first_row))
    def _():
        for x_home in (0, 1):
            pl.semaphore_signal(
                barrier, inc=1, device_id=at(0, 0, x_home, z, tp), device_id_type=MESH
            )
        pl.semaphore_wait(barrier, 11)

    size = 256 // CHUNKS
    spans = [pl.ds(c * size, size) for c in range(CHUNKS)]
    x_copies = [
        remote(x_hbm.at[:, s], x_far.at[:, s], x_send.at[c], x_recv.at[c], partner)
        for c, s in enumerate(spans)
    ]
    for copy in x_copies:
        copy.start()
    load_x = pltpu.make_async_copy(x_hbm, x_own, load_sem.at[0])
    load_kv = pltpu.make_async_copy(wkv_hbm, wkv_raw, load_sem.at[1])
    load_q = pltpu.make_async_copy(wq_hbm, wq_raw, load_sem.at[2])
    load_kv.start()
    load_q.start()
    load_x.start()
    load_kv.wait()

    @pl.loop(0, 4)
    def _(block):
        rows = pl.ds(pl.multiple_of(block * 512, 512), 512)
        spread[...] = wkv_raw[rows].reshape(4096, 128).astype(jnp.float32)
        kept = pl.ds(pl.multiple_of(block * 1024, 1024), 1024)
        for g in range(2):
            for c in range(2):
                at_column = (g * 2 + c) * 128
                wkv[kept, at_column:at_column + 128] = spread[
                    pl.ds(c * 2 + g, 1024, stride=4), :
                ].astype(jnp.bfloat16)

    load_q.wait()

    @pl.loop(0, 8)
    def _(block):
        rows = pl.ds(pl.multiple_of(block * 512, 512), 512)
        spread[...] = wq_raw[rows].reshape(4096, 128).astype(jnp.float32)
        for h in range(8):
            wq[rows, h * 128:(h + 1) * 128] = spread[pl.ds(h, 512, stride=8), :].astype(
                jnp.bfloat16
            )

    load_x.wait()
    own_rows = pl.ds(pl.multiple_of(tp * 2048, 2048), 2048)
    far_rows = pl.ds(pl.multiple_of((1 - tp) * 2048, 2048), 2048)

    def columns(n):
        return pl.ds(pl.multiple_of(n * 256, 256), 256)

    @pl.loop(0, 2)
    def _(n):
        acc_kv[:, :, columns(n)] = jnp.dot(
            x_own[...].reshape(512, 2048),
            wkv[own_rows, columns(n)],
            preferred_element_type=jnp.float32,
        ).reshape(2, 256, 256)

    @pl.loop(0, 4)
    def _(n):
        acc_q[:, :, columns(n)] = jnp.dot(
            x_own[...].reshape(512, 2048),
            wq[own_rows, columns(n)],
            preferred_element_type=jnp.float32,
        ).reshape(2, 256, 256)

    slab_start = (core * 32 + y * 8 + x * 4 + z) * 256
    pending = []
    kv_copies, q_copies, keeps, a_copies, b_copies, aa_copies, bb_copies = [], [], [], [], [], [], []

    def pass_on(c):
        s = spans[c]
        a_copies[c].wait_recv()
        aa = remote(
            kv_all.at[8:12, s], kv_all.at[0:4, s], aa_send.at[c], aa_recv.at[c], ahead
        )
        aa.start()
        aa_copies.append(aa)
        b_copies[c].wait_recv()
        bb = remote(
            kv_all.at[12:16, s], kv_all.at[4:8, s], bb_send.at[c], bb_recv.at[c], ahead
        )
        bb.start()
        bb_copies.append(bb)

    for c in range(CHUNKS):
        s = spans[c]
        x_copies[c].wait_recv()
        cosine, sine = cos_ref[s, :], sin_ref[s, :]

        @pl.loop(0, 2)
        def _(n):
            total = jnp.dot(
                x_far[:, s].reshape(2 * size, 2048),
                wkv[far_rows, columns(n)],
                preferred_element_type=jnp.float32,
            )
            for r in range(2):
                block = total[r * size:(r + 1) * size] + acc_kv[r, s, columns(n)]
                keys = turned(block[:, :128], cosine, sine).astype(jnp.bfloat16)
                both = jnp.concatenate([keys, block[:, 128:].astype(jnp.bfloat16)], axis=1)
                kv_stage[r * 2 + n, s, :] = both
                position = (
                    slab_start + c * size + lax.broadcasted_iota(jnp.int32, (size, 256), 0)
                )
                cache_stage[r, n, s, :] = jnp.where(
                    position < lens[r], both.astype(jnp.float32), 0.0
                ).astype(jnp.bfloat16)

        for d in (1, 2, 3):
            target = lax.rem(z + d, 4)
            copy = remote(
                kv_stage.at[target, s], kv_all.at[16 + z, s],
                kv_send.at[c, d - 1], kv_recv.at[c, d - 1], peers[d - 1],
            )
            copy.start()
            kv_copies.append(copy)
        keep = pltpu.make_async_copy(kv_stage.at[z, s], kv_all.at[16 + z, s], kv_keep.at[c])
        keep.start()

        @pl.loop(0, 4)
        def _(n):
            total = jnp.dot(
                x_far[:, s].reshape(2 * size, 2048),
                wq[far_rows, columns(n)],
                preferred_element_type=jnp.float32,
            )
            for r in range(2):
                block = total[r * size:(r + 1) * size] + acc_q[r, s, columns(n)]
                for k in range(2):
                    head = turned(block[:, k * 128:(k + 1) * 128], cosine, sine)
                    q_stage[r * 2 + n // 2, lax.rem(n, 2) * 2 + k, s, :] = head.astype(
                        jnp.bfloat16
                    )

        for d in (1, 2, 3):
            target = lax.rem(z + d, 4)
            copy = remote(
                q_stage.at[target, :, s], q_all.at[z, :, s],
                q_send.at[c, d - 1], q_recv.at[c, d - 1], peers[d - 1],
            )
            copy.start()
            q_copies.append(copy)
        q_own = pltpu.make_async_copy(q_stage.at[z, :, s], q_all.at[z, :, s], q_keep.at[c])
        q_own.start()
        keeps.append(q_own)

        keep.wait()
        for d in range(3):
            kv_copies[c * 3 + d].wait_recv()
        a = remote(kv_all.at[16:20, s], kv_all.at[8:12, s], a_send.at[c], a_recv.at[c], ahead)
        b = remote(kv_all.at[16:20, s], kv_all.at[12:16, s], b_send.at[c], b_recv.at[c], side)
        a.start()
        b.start()
        a_copies.append(a)
        b_copies.append(b)
        if c >= 1:
            pass_on(c - 1)

    cache_copy = remote(
        cache_stage.at[:, 1 - core], cache_out.at[:, core], c_send.at[0], c_recv.at[0], twin
    )
    cache_copy.start()
    cache_keep = pltpu.make_async_copy(
        cache_stage.at[:, core], cache_out.at[:, core], c_keep.at[0]
    )
    cache_keep.start()

    sink_sends = [
        remote(
            sink_stage, sink_all.at[x], s_send.at[n - 1], s_recv.at[x], sink_target(n)
        )
        for n in range(1, 16)
    ]
    sink_keep = pltpu.make_async_copy(sink_stage, sink_all.at[x], s_keep.at[0])

    @pl.when(first_row)
    def _():
        sink_stage[...] = jnp.dot(
            hot_ref[...], kv_all[16:20].reshape(1024, 256), preferred_element_type=jnp.float32
        ).astype(jnp.bfloat16)
        for copy in sink_sends:
            copy.start()
        sink_keep.start()

    for copy in keeps:
        copy.wait()
    for copy in q_copies:
        copy.wait_recv()
    group = row * 2 + x
    request = z // 2
    length = lens[request]
    key_at = lax.broadcasted_iota(jnp.int32, (256, 256), 0)
    query_at = lax.broadcasted_iota(jnp.int32, (256, 256), 1)

    def turn_values(first, count):
        @pl.loop(first, first + count)
        def _(slab):
            values[slab, :128, :] = (
                kv_all[slab, :, 128:].astype(jnp.float32).T.astype(jnp.bfloat16)
            )
            values[slab, 128:, :] = jnp.ones((16, 256), jnp.bfloat16)

    def rescale(j, h, new, gained):
        factor = jnp.exp2((peak[j, h] - new) * SCALE)
        peak[j, h] = new
        total[j, h] = (total[j, h].reshape(18, 8, 256) * factor[None]).reshape(144, 256) + gained

    def top_of(block):
        return jnp.broadcast_to(jnp.max(block, axis=0, keepdims=True), (8, 256))

    def fold(j, items):
        tops = []
        for h in range(4):
            top = peak[j, h]
            for i, (slab, visible) in enumerate(items):
                block = lax.dot_general(
                    kv_all[slab, :, :128], q_all[j, h], (((1,), (1,)), ((), ())),
                    preferred_element_type=jnp.float32,
                )
                if visible is not None:
                    block = jnp.where(visible, block, NEG_FILL)
                scores[h, i] = block
                top = jnp.maximum(top, jnp.max(block.reshape(32, 8, 256), axis=0))
            tops.append(top_of(top))
        for h in range(4):
            shift = tops[h] * SCALE
            gained = None
            for i, (slab, _) in enumerate(items):
                weights = jnp.exp2(
                    (scores[h, i] * SCALE).reshape(32, 8, 256) - shift[None]
                ).reshape(256, 256)
                part = jnp.dot(
                    values[slab], weights.astype(jnp.bfloat16),
                    preferred_element_type=jnp.float32,
                )
                gained = part if gained is None else gained + part
            rescale(j, h, tops[h], gained)

    turn_values(16, 4)

    @pl.loop(0, 4)
    def _(j):
        for h in range(4):
            peak[j, h] = jnp.full((8, 256), NEG_FILL, jnp.float32)
            total[j, h] = jnp.zeros((144, 256), jnp.float32)
        fold(j, [(16 + j, key_at <= query_at)])

    pass_on(CHUNKS - 1)
    turn_values(8, 8)

    for back in (1, 2):
        @pl.when(group >= back)
        def _():
            @pl.loop(0, 4)
            def _(j):
                fold(j, [(20 - 4 * back - 4 + i, None) for i in range(4)])

    for copy in aa_copies + bb_copies:
        copy.wait_recv()
    turn_values(0, 8)
    @pl.when(first_row)
    def _():
        sink_keep.wait()
        for copy in sink_sends:
            copy.wait_send()
        remote(sink_stage, sink_all.at[1 - x], s_send.at[0], s_recv.at[1 - x], partner).wait_recv()

    @pl.when(jnp.logical_not(first_row))
    def _():
        for home in (0, 1):
            remote(
                sink_stage, sink_all.at[home], s_send.at[0], s_recv.at[home], partner
            ).wait_recv()
    sink_kv = (sink_all[0].astype(jnp.float32) + sink_all[1].astype(jnp.float32)).astype(
        jnp.bfloat16
    )
    sink_values[:128, :] = (
        jnp.concatenate(
            [sink_kv[:, 128:].astype(jnp.float32), jnp.zeros((112, 128), jnp.float32)], axis=0
        ).T.astype(jnp.bfloat16)
    )
    sink_values[128:, :] = jnp.ones((16, 128), jnp.bfloat16)
    out_columns = pl.ds(pl.multiple_of(lax.rem(z, 2) * 512, 512), 512)

    @pl.loop(0, 4)
    def _(turn):
        j = lax.rem(z + 1 + turn, 4)

        @pl.when(group >= 3)
        def _():
            fold(j, [(4 + i, None) for i in range(4)])

        @pl.when(group >= 4)
        def _():
            edges = [(jnp.where(t < j, 16 + t, t + 1), None) for t in range(3)]
            fold(j, edges + [(j, key_at > query_at)])

        @pl.when(group < 4)
        def _():
            def inner(t, carry):
                fold(j, [(16 + t, None)])
                return carry

            lax.fori_loop(0, j, inner, 0)

        first = (group * 4 + j) * 256
        far = first + query_at[:16] - sink_pos[...] >= WINDOW
        for h in range(4):
            block = lax.dot_general(
                sink_kv[:, :128], q_all[j, h], (((1,), (1,)), ((), ())),
                preferred_element_type=jnp.float32,
            )
            block = jnp.where(far, block, NEG_FILL)
            top = top_of(
                jnp.maximum(peak[j, h], jnp.max(block.reshape(2, 8, 256), axis=0))
            )
            weights = jnp.exp2((block * SCALE).reshape(2, 8, 256) - (top * SCALE)[None])
            weights = jnp.concatenate(
                [weights.reshape(16, 256), jnp.zeros((112, 256), jnp.float32)], axis=0
            )
            rescale(
                j, h, top,
                jnp.dot(
                    sink_values[...], weights.astype(jnp.bfloat16),
                    preferred_element_type=jnp.float32,
                ),
            )
            mixed = (total[j, h, :128] / total[j, h, 128:129]).T
            live = first + lax.broadcasted_iota(jnp.int32, (256, 128), 0) < length
            stage[turn, :, h * 128:(h + 1) * 128] = jnp.where(live, mixed, 0.0).astype(
                jnp.bfloat16
            )

        home = out_ref.at[request, :, out_columns]

        @pl.when(turn < 3)
        def _():
            remote(
                stage.at[turn], home, o_send.at[turn], o_recv.at[turn],
                at(core, y, x, j, tp),
            ).start()

        @pl.when(turn == 3)
        def _():
            pltpu.make_async_copy(stage.at[turn], home, o_keep.at[0]).start()

    pltpu.make_async_copy(
        stage.at[3], out_ref.at[request, :, out_columns], o_keep.at[0]
    ).wait()
    for turn in range(3):
        source = lax.rem(z + 3 - turn, 4)
        landed = out_ref.at[
            source // 2, :, pl.ds(pl.multiple_of(lax.rem(source, 2) * 512, 512), 512)
        ]
        remote(
            stage.at[turn], landed, o_send.at[turn], o_recv.at[turn], peers[turn]
        ).wait()
    cache_keep.wait()
    cache_copy.wait()
    for copy in aa_copies + bb_copies + q_copies + kv_copies + a_copies + b_copies + x_copies:
        copy.wait_send()


def dma(*shape):
    return pltpu.SemaphoreType.DMA(shape)


def per_device(prompt_states, q_weight, kv_weight, lengths, sink_positions):
    bf16 = jnp.bfloat16
    core, y, x, z, tp = place()
    group = (core * 4 + y) * 2 + x
    kv_rows = kv_weight.reshape(2048, 8, 128)
    positions = (group * 4 + z) * 256 + jnp.arange(256, dtype=jnp.int32)
    ladder = jnp.arange(64, dtype=jnp.float32) * (2.0 / 128)
    inv_freq = jnp.exp(-math.log(ROPE_BASE) * ladder)
    angles = positions.astype(jnp.float32)[:, None] * inv_freq[None, :]
    cosine, sine = jnp.cos(angles), jnp.sin(angles)
    cos_table = jnp.concatenate([cosine, cosine], axis=1)
    sin_table = jnp.concatenate([-sine, sine], axis=1)
    sinks = jnp.where(z < 2, sink_positions[0], sink_positions[1])
    group_pos = group * 1024 + jnp.arange(1024, dtype=jnp.int32)
    hot = (sinks[:, None] == group_pos[None, :]).astype(bf16)
    hot = jnp.pad(hot, ((0, 12), (0, 0)))
    earlier = jnp.arange(4)[None, :] < jnp.arange(4)[:, None]
    repeated = jnp.any((sinks[:, None] == sinks[None, :]) & earlier, axis=1)
    sink_column = jnp.pad(jnp.where(repeated, FAR, sinks), (0, 12), constant_values=FAR)
    sink_column = jnp.broadcast_to(sink_column[:, None], (16, 256))

    anyspace = pl.BlockSpec(memory_space=pl.ANY)
    vmem = pl.BlockSpec(memory_space=pltpu.VMEM)
    smem = pl.BlockSpec(memory_space=pltpu.SMEM)
    shape = jax.ShapeDtypeStruct
    f32 = jnp.float32
    attended, cache = pl.pallas_call(
        layer_kernel,
        out_shape=(shape((2, 256, 1024), bf16), shape((2, 2, 256, 256), bf16)),
        in_specs=[smem, anyspace, anyspace, anyspace, vmem, vmem, vmem, vmem],
        out_specs=(anyspace, anyspace),
        scratch_shapes=[
            pltpu.VMEM((2, 256, 2048), bf16),
            pltpu.VMEM((2, 256, 2048), bf16),
            pltpu.VMEM((4096, 8, 128), bf16),
            pltpu.VMEM((2048, 8, 128), bf16),
            pltpu.VMEM((4096, 128), f32),
            pltpu.VMEM((4096, 1024), bf16),
            pltpu.VMEM((4096, 512), bf16),
            pltpu.VMEM((2, 256, 1024), f32),
            pltpu.VMEM((2, 256, 512), f32),
            pltpu.VMEM((4, 4, 256, 128), bf16),
            pltpu.VMEM((4, 256, 256), bf16),
            pltpu.VMEM((2, 2, 256, 256), bf16),
            pltpu.VMEM((4, 4, 256, 128), bf16),
            pltpu.VMEM((20, 256, 256), bf16),
            pltpu.VMEM((2, 16, 256), bf16),
            pltpu.VMEM((16, 256), bf16),
            pltpu.VMEM((20, 144, 256), bf16),
            pltpu.VMEM((144, 128), bf16),
            pltpu.VMEM((4, 4, 8, 256), f32),
            pltpu.VMEM((4, 4, 144, 256), f32),
            pltpu.VMEM((4, 4, 256, 256), f32),
            pltpu.VMEM((4, 256, 512), bf16),
            dma(CHUNKS), dma(CHUNKS), dma(3),
            dma(CHUNKS, 3), dma(CHUNKS, 3), dma(CHUNKS),
            dma(CHUNKS, 3), dma(CHUNKS, 3), dma(CHUNKS),
            dma(CHUNKS), dma(CHUNKS), dma(CHUNKS), dma(CHUNKS),
            dma(CHUNKS), dma(CHUNKS), dma(CHUNKS), dma(CHUNKS),
            dma(1), dma(1), dma(1), dma(15), dma(2), dma(1),
            dma(3), dma(3), dma(1),
        ],
        compiler_params=pltpu.CompilerParams(
            collective_id=0, has_side_effects=True, vmem_limit_bytes=VMEM_BYTES
        ),
    )(lengths, prompt_states, q_weight, kv_rows, cos_table, sin_table, hot, sink_column)
    return attended, cache.reshape(2, 1, 2, 1, 256, 256)


def solution(mesh):
    placed = (
        P(None, ("grp", "seq"), "tp"),
        P(None, "tp", None),
        P(None, None, "tp", None),
        P(),
        P(),
    )
    return jax.shard_map(
        per_device,
        mesh=mesh,
        in_specs=placed,
        out_specs=(P(None, ("grp", "seq"), "tp"), P(None, ("tp", "grp"), None, "seq", None, None)),
        check_vma=False,
    )
```

```python
import math

import jax
import jax.numpy as jnp
from jax import lax
from jax.experimental import pallas as pl
from jax.experimental.pallas import tpu as pltpu
from jax.sharding import PartitionSpec as P

WINDOW = 4096
ROPE_BASE = 10000.0
NEG_FILL = -1e30
FAR = 1 << 30
MESH = pl.DeviceIdType.MESH
CHUNKS = 4
EARLY_SIDE = 2
VMEM_BYTES = 60 * 2**20


def place():
    core, seq, tp = lax.axis_index("grp"), lax.axis_index("seq"), lax.axis_index("tp")
    return core, seq // 8, lax.rem(seq // 4, 2), lax.rem(seq, 4), tp


def at(core, y, x, z, tp):
    return (core, y * 8 + x * 4 + z, tp)


def next_row(core, y):
    wraps = (y + 1) // 4
    return lax.rem(core + wraps, 2), lax.rem(y + 1, 4)


def previous_row(core, y):
    wraps = (4 - y) // 4
    return lax.rem(core + wraps, 2), lax.rem(y + 3, 4)


def remote(src, dst, send_sem, recv_sem, target):
    return pltpu.make_async_remote_copy(
        src_ref=src,
        dst_ref=dst,
        send_sem=send_sem,
        recv_sem=recv_sem,
        device_id=target,
        device_id_type=MESH,
    )


def turned(block, cosine, sine):
    return block * cosine + pltpu.roll(block, 64, 1) * sine


SCALE = math.log2(math.e) / math.sqrt(128.0)


def layer_kernel(
    lens, sinks, x_hbm, wq_hbm, wkv_hbm, cos_ref, sin_ref,
    out_ref, cache_out,
    x_own, x_far, wq_raw, wkv_raw, spread, wq, wkv, acc_q, acc_kv, q_stage, kv_stage, cache_stage,
    q_all, kv_all, sink_all, sink_stage, values, sink_values, peak, total, scores, stage,
    x_send, x_recv, load_sem, kv_send, kv_recv, kv_keep, q_send, q_recv, q_keep,
    a_send, a_recv, b_send, b_recv, aa_send, aa_recv, bb_send, bb_recv,
    c_send, c_recv, c_keep, s_send, s_recv, s_keep, o_send, o_recv, o_keep,
):
    core, y, x, z, tp = place()
    up, down = next_row(core, y), previous_row(core, y)
    ahead, behind = at(*up, x, z, tp), at(*down, x, z, tp)
    partner = at(core, y, x, z, 1 - tp)
    twin = at(1 - core, y, x, z, tp)
    side = at(core, y, 1 - x, z, tp)
    beyond = at(lax.rem(core + (y + 2) // 4, 2), lax.rem(y + 2, 4), x, z, tp)
    before = at(lax.rem(core + (5 - y) // 4, 2), lax.rem(y + 2, 4), x, z, tp)
    first_row = (core + y) == 0
    row = core * 4 + y
    peers = [at(core, y, x, lax.rem(z + d, 4), tp) for d in (1, 2, 3)]

    barrier = pltpu.get_barrier_semaphore()
    for other in [partner, twin, ahead, behind, beyond, before, side, *peers]:
        pl.semaphore_signal(barrier, inc=1, device_id=other, device_id_type=MESH)

    def sink_target(n):
        slot = lax.rem(row * 2 + x + n, 16)
        return at(slot // 8, lax.rem(slot // 2, 4), lax.rem(slot, 2), z, tp)

    @pl.when(first_row)
    def _():
        for n in range(1, 16):
            pl.semaphore_signal(barrier, inc=1, device_id=sink_target(n), device_id_type=MESH)
        pl.semaphore_wait(barrier, 25)

    @pl.when(jnp.logical_not(first_row))
    def _():
        for x_home in (0, 1):
            pl.semaphore_signal(
                barrier, inc=1, device_id=at(0, 0, x_home, z, tp), device_id_type=MESH
            )
        pl.semaphore_wait(barrier, 12)

    request = z // 2
    marks = [sinks[request, n] for n in range(4)]
    fresh = []
    for n in range(4):
        mark = marks[n]
        for earlier in marks[:n]:
            mark = jnp.where(marks[n] == earlier, FAR, mark)
        fresh.append(mark)
    size = 256 // CHUNKS
    spans = [pl.ds(c * size, size) for c in range(CHUNKS)]
    x_copies = [
        remote(x_hbm.at[:, s], x_far.at[:, s], x_send.at[c], x_recv.at[c], partner)
        for c, s in enumerate(spans)
    ]
    for copy in x_copies:
        copy.start()
    load_x = pltpu.make_async_copy(x_hbm, x_own, load_sem.at[0])
    load_kv = pltpu.make_async_copy(wkv_hbm, wkv_raw, load_sem.at[1])
    load_q = pltpu.make_async_copy(wq_hbm, wq_raw, load_sem.at[2])
    load_kv.start()
    load_q.start()
    load_x.start()
    load_kv.wait()

    @pl.loop(0, 4)
    def _(block):
        rows = pl.ds(pl.multiple_of(block * 512, 512), 512)
        spread[...] = wkv_raw[rows].reshape(4096, 128).astype(jnp.float32)
        kept = pl.ds(pl.multiple_of(block * 1024, 1024), 1024)
        for g in range(2):
            for c in range(2):
                at_column = (g * 2 + c) * 128
                wkv[kept, at_column:at_column + 128] = spread[
                    pl.ds(c * 2 + g, 1024, stride=4), :
                ].astype(jnp.bfloat16)

    load_q.wait()

    @pl.loop(0, 8)
    def _(block):
        rows = pl.ds(pl.multiple_of(block * 512, 512), 512)
        spread[...] = wq_raw[rows].reshape(4096, 128).astype(jnp.float32)
        for h in range(8):
            wq[rows, h * 128:(h + 1) * 128] = spread[pl.ds(h, 512, stride=8), :].astype(
                jnp.bfloat16
            )

    load_x.wait()
    own_rows = pl.ds(pl.multiple_of(tp * 2048, 2048), 2048)
    far_rows = pl.ds(pl.multiple_of((1 - tp) * 2048, 2048), 2048)

    def columns(n):
        return pl.ds(pl.multiple_of(n * 256, 256), 256)

    @pl.loop(0, 2)
    def _(n):
        acc_kv[:, :, columns(n)] = jnp.dot(
            x_own[...].reshape(512, 2048),
            wkv[own_rows, columns(n)],
            preferred_element_type=jnp.float32,
        ).reshape(2, 256, 256)

    @pl.loop(0, 4)
    def _(n):
        acc_q[:, :, columns(n)] = jnp.dot(
            x_own[...].reshape(512, 2048),
            wq[own_rows, columns(n)],
            preferred_element_type=jnp.float32,
        ).reshape(2, 256, 256)

    slab_start = (core * 32 + y * 8 + x * 4 + z) * 256
    pending = []
    kv_copies, q_copies, keeps, a_copies, b_copies, aa_copies = [], [], [], [], [], []

    side_source = pl.ds(16 - 8 * x, 4)

    def to_side(c):
        s = spans[c]
        a_copies[c].wait_recv()
        b = remote(
            kv_all.at[side_source, s], kv_all.at[12:16, s], b_send.at[c], b_recv.at[c], side
        )
        b.start()
        b_copies.append(b)

    def from_side(c):
        s = pl.ds(pl.multiple_of(c * size, size), size)
        remote(
            kv_all.at[side_source, s], kv_all.at[12:16, s], b_send.at[c], b_recv.at[c], side
        ).wait_recv()
        remote(
            kv_all.at[12:16, s], kv_all.at[4:8, s], bb_send.at[c], bb_recv.at[c], ahead
        ).start()

    for c in range(CHUNKS):
        s = spans[c]
        x_copies[c].wait_recv()
        if c == 2:
            for early in range(EARLY_SIDE):
                to_side(early)
        if c == CHUNKS - 1:
            for late in range(EARLY_SIDE, CHUNKS - 1):
                to_side(late)
        cosine, sine = cos_ref[s, :], sin_ref[s, :]

        @pl.loop(0, 2)
        def _(n):
            total = jnp.dot(
                x_far[:, s].reshape(2 * size, 2048),
                wkv[far_rows, columns(n)],
                preferred_element_type=jnp.float32,
            )
            for r in range(2):
                block = total[r * size:(r + 1) * size] + acc_kv[r, s, columns(n)]
                keys = turned(block[:, :128], cosine, sine).astype(jnp.bfloat16)
                both = jnp.concatenate([keys, block[:, 128:].astype(jnp.bfloat16)], axis=1)
                kv_stage[r * 2 + n, s, :] = both
                position = (
                    slab_start + c * size + lax.broadcasted_iota(jnp.int32, (size, 256), 0)
                )
                cache_stage[r, n, s, :] = jnp.where(
                    position < lens[r], both.astype(jnp.float32), 0.0
                ).astype(jnp.bfloat16)

        for d in (1, 2, 3):
            target = lax.rem(z + d, 4)
            copy = remote(
                kv_stage.at[target, s], kv_all.at[16 + z, s],
                kv_send.at[c, d - 1], kv_recv.at[c, d - 1], peers[d - 1],
            )
            copy.start()
            kv_copies.append(copy)
        keep = pltpu.make_async_copy(kv_stage.at[z, s], kv_all.at[16 + z, s], kv_keep.at[c])
        keep.start()

        @pl.loop(0, 4)
        def _(n):
            total = jnp.dot(
                x_far[:, s].reshape(2 * size, 2048),
                wq[far_rows, columns(n)],
                preferred_element_type=jnp.float32,
            )
            for r in range(2):
                block = total[r * size:(r + 1) * size] + acc_q[r, s, columns(n)]
                for k in range(2):
                    head = turned(block[:, k * 128:(k + 1) * 128], cosine, sine)
                    q_stage[r * 2 + n // 2, lax.rem(n, 2) * 2 + k, s, :] = head.astype(
                        jnp.bfloat16
                    )

        for d in (1, 2, 3):
            target = lax.rem(z + d, 4)
            copy = remote(
                q_stage.at[target, :, s], q_all.at[z, :, s],
                q_send.at[c, d - 1], q_recv.at[c, d - 1], peers[d - 1],
            )
            copy.start()
            q_copies.append(copy)
        q_own = pltpu.make_async_copy(q_stage.at[z, :, s], q_all.at[z, :, s], q_keep.at[c])
        q_own.start()
        keeps.append(q_own)

        keep.wait()
        for d in range(3):
            kv_copies[c * 3 + d].wait_recv()
        a = remote(kv_all.at[16:20, s], kv_all.at[8:12, s], a_send.at[c], a_recv.at[c], ahead)
        a.start()
        a_copies.append(a)
        aa = remote(kv_all.at[16:20, s], kv_all.at[0:4, s], aa_send.at[c], aa_recv.at[c], beyond)
        aa.start()
        aa_copies.append(aa)
        if c == CHUNKS - 1:
            for early in range(EARLY_SIDE):
                from_side(early)

    cache_copy = remote(
        cache_stage.at[:, 1 - core], cache_out.at[:, core], c_send.at[0], c_recv.at[0], twin
    )
    cache_copy.start()
    cache_keep = pltpu.make_async_copy(
        cache_stage.at[:, core], cache_out.at[:, core], c_keep.at[0]
    )
    cache_keep.start()

    sink_sends = [
        remote(
            sink_stage, sink_all.at[x], s_send.at[n - 1], s_recv.at[x], sink_target(n)
        )
        for n in range(1, 16)
    ]
    sink_keep = pltpu.make_async_copy(sink_stage, sink_all.at[x], s_keep.at[0])

    @pl.when(first_row)
    def _():
        mark_row = lax.broadcasted_iota(jnp.int32, (16, 1024), 0)
        token = row * 2048 + x * 1024 + lax.broadcasted_iota(jnp.int32, (16, 1024), 1)
        wanted = jnp.full((16, 1024), FAR, jnp.int32)
        for n in range(4):
            wanted = jnp.where(mark_row == n, marks[n], wanted)
        hot = jnp.where(token == wanted, 1.0, 0.0).astype(jnp.bfloat16)
        sink_stage[...] = jnp.dot(
            hot, kv_all[16:20].reshape(1024, 256), preferred_element_type=jnp.float32
        ).astype(jnp.bfloat16)
        for copy in sink_sends:
            copy.start()
        sink_keep.start()

    for copy in keeps:
        copy.wait()
    for copy in q_copies:
        copy.wait_recv()
    group = row * 2 + x
    length = lens[request]
    key_at = lax.broadcasted_iota(jnp.int32, (256, 256), 0)
    query_at = lax.broadcasted_iota(jnp.int32, (256, 256), 1)

    def turn_values(first, count):
        @pl.loop(first, first + count)
        def _(slab):
            values[slab, :128, :] = (
                kv_all[slab, :, 128:].astype(jnp.float32).T.astype(jnp.bfloat16)
            )
            values[slab, 128:, :] = jnp.ones((16, 256), jnp.bfloat16)

    def rescale(j, h, new, gained):
        factor = jnp.exp2((peak[j, h] - new) * SCALE)
        peak[j, h] = new
        total[j, h] = (total[j, h].reshape(18, 8, 256) * factor[None]).reshape(144, 256) + gained

    def top_of(block):
        return jnp.broadcast_to(jnp.max(block, axis=0, keepdims=True), (8, 256))

    def fold(j, items):
        tops = []
        for h in range(4):
            top = peak[j, h]
            for i, (slab, visible) in enumerate(items):
                block = lax.dot_general(
                    kv_all[slab, :, :128], q_all[j, h], (((1,), (1,)), ((), ())),
                    preferred_element_type=jnp.float32,
                )
                if visible is not None:
                    block = jnp.where(visible, block, NEG_FILL)
                scores[h, i] = block
                top = jnp.maximum(top, jnp.max(block.reshape(32, 8, 256), axis=0))
            tops.append(top_of(top))
        for h in range(4):
            shift = tops[h] * SCALE
            gained = None
            for i, (slab, _) in enumerate(items):
                weights = jnp.exp2(
                    (scores[h, i] * SCALE).reshape(32, 8, 256) - shift[None]
                ).reshape(256, 256)
                part = jnp.dot(
                    values[slab], weights.astype(jnp.bfloat16),
                    preferred_element_type=jnp.float32,
                )
                gained = part if gained is None else gained + part
            rescale(j, h, tops[h], gained)

    turn_values(16, 4)

    @pl.loop(0, 4)
    def _(j):
        for h in range(4):
            peak[j, h] = jnp.full((8, 256), NEG_FILL, jnp.float32)
            total[j, h] = jnp.zeros((144, 256), jnp.float32)
        fold(j, [(16 + j, key_at <= query_at)])

    to_side(CHUNKS - 1)
    turn_values(8, 4)

    @pl.when(group >= 2)
    def _():
        @pl.loop(0, 4)
        def _(j):
            fold(j, [(8 + i, None) for i in range(4)])

    for copy in aa_copies:
        copy.wait_recv()
    turn_values(0, 4)

    @pl.loop(0, CHUNKS)
    def _(j):
        @pl.when(j < CHUNKS - EARLY_SIDE)
        def _():
            from_side(j + EARLY_SIDE)

        @pl.when(group >= 4)
        def _():
            edges = [(jnp.where(t < j, 16 + t, t + 1), None) for t in range(3)]
            fold(j, edges + [(j, key_at > query_at)])

        @pl.when(group < 4)
        def _():
            def inner(t, carry):
                fold(j, [(16 + t, None)])
                return carry

            lax.fori_loop(0, j, inner, 0)

    turn_values(12, 4)

    @pl.when(group >= 1)
    def _():
        @pl.loop(0, 4)
        def _(j):
            fold(j, [(12 + i, None) for i in range(4)])

    bb_copies = [
        remote(kv_all.at[12:16, s], kv_all.at[4:8, s], bb_send.at[c], bb_recv.at[c], ahead)
        for c, s in enumerate(spans)
    ]
    for copy in bb_copies:
        copy.wait_recv()
    turn_values(4, 4)
    @pl.when(first_row)
    def _():
        sink_keep.wait()
        for copy in sink_sends:
            copy.wait_send()
        remote(sink_stage, sink_all.at[1 - x], s_send.at[0], s_recv.at[1 - x], partner).wait_recv()

    @pl.when(jnp.logical_not(first_row))
    def _():
        for home in (0, 1):
            remote(
                sink_stage, sink_all.at[home], s_send.at[0], s_recv.at[home], partner
            ).wait_recv()
    sink_kv = (sink_all[0].astype(jnp.float32) + sink_all[1].astype(jnp.float32)).astype(
        jnp.bfloat16
    )
    sink_values[:128, :] = (
        jnp.concatenate(
            [sink_kv[:, 128:].astype(jnp.float32), jnp.zeros((112, 128), jnp.float32)], axis=0
        ).T.astype(jnp.bfloat16)
    )
    sink_values[128:, :] = jnp.ones((16, 128), jnp.bfloat16)
    mark_at = lax.broadcasted_iota(jnp.int32, (16, 256), 0)
    sink_at = jnp.full((16, 256), FAR, jnp.int32)
    for n in range(4):
        sink_at = jnp.where(mark_at == n, fresh[n], sink_at)
    out_columns = pl.ds(pl.multiple_of(lax.rem(z, 2) * 512, 512), 512)

    @pl.loop(0, 4)
    def _(turn):
        j = lax.rem(z + 1 + turn, 4)

        @pl.when(group >= 3)
        def _():
            fold(j, [(4 + i, None) for i in range(4)])

        first = (group * 4 + j) * 256
        far = first + query_at[:16] - sink_at >= WINDOW
        for h in range(4):
            block = lax.dot_general(
                sink_kv[:, :128], q_all[j, h], (((1,), (1,)), ((), ())),
                preferred_element_type=jnp.float32,
            )
            block = jnp.where(far, block, NEG_FILL)
            top = top_of(
                jnp.maximum(peak[j, h], jnp.max(block.reshape(2, 8, 256), axis=0))
            )
            weights = jnp.exp2((block * SCALE).reshape(2, 8, 256) - (top * SCALE)[None])
            weights = jnp.concatenate(
                [weights.reshape(16, 256), jnp.zeros((112, 256), jnp.float32)], axis=0
            )
            rescale(
                j, h, top,
                jnp.dot(
                    sink_values[...], weights.astype(jnp.bfloat16),
                    preferred_element_type=jnp.float32,
                ),
            )
            mixed = (total[j, h, :128] / total[j, h, 128:129]).T
            live = first + lax.broadcasted_iota(jnp.int32, (256, 128), 0) < length
            stage[turn, :, h * 128:(h + 1) * 128] = jnp.where(live, mixed, 0.0).astype(
                jnp.bfloat16
            )

        home = out_ref.at[request, :, out_columns]

        @pl.when(turn < 3)
        def _():
            remote(
                stage.at[turn], home, o_send.at[turn], o_recv.at[turn],
                at(core, y, x, j, tp),
            ).start()

        @pl.when(turn == 3)
        def _():
            pltpu.make_async_copy(stage.at[turn], home, o_keep.at[0]).start()

    pltpu.make_async_copy(
        stage.at[3], out_ref.at[request, :, out_columns], o_keep.at[0]
    ).wait()
    for turn in range(3):
        source = lax.rem(z + 3 - turn, 4)
        landed = out_ref.at[
            source // 2, :, pl.ds(pl.multiple_of(lax.rem(source, 2) * 512, 512), 512)
        ]
        remote(
            stage.at[turn], landed, o_send.at[turn], o_recv.at[turn], peers[turn]
        ).wait()
    cache_keep.wait()
    cache_copy.wait()
    for copy in aa_copies + bb_copies + q_copies + kv_copies + a_copies + b_copies + x_copies:
        copy.wait_send()


def dma(*shape):
    return pltpu.SemaphoreType.DMA(shape)


def per_device(prompt_states, q_weight, kv_weight, lengths, sink_positions):
    bf16 = jnp.bfloat16
    core, y, x, z, tp = place()
    group = (core * 4 + y) * 2 + x
    kv_rows = kv_weight.reshape(2048, 8, 128)
    positions = (group * 4 + z) * 256 + jnp.arange(256, dtype=jnp.int32)
    ladder = jnp.arange(64, dtype=jnp.float32) * (2.0 / 128)
    inv_freq = jnp.exp(-math.log(ROPE_BASE) * ladder)
    angles = positions.astype(jnp.float32)[:, None] * inv_freq[None, :]
    cosine, sine = jnp.cos(angles), jnp.sin(angles)
    cos_table = jnp.concatenate([cosine, cosine], axis=1)
    sin_table = jnp.concatenate([-sine, sine], axis=1)
    anyspace = pl.BlockSpec(memory_space=pl.ANY)
    vmem = pl.BlockSpec(memory_space=pltpu.VMEM)
    smem = pl.BlockSpec(memory_space=pltpu.SMEM)
    shape = jax.ShapeDtypeStruct
    f32 = jnp.float32
    attended, cache = pl.pallas_call(
        layer_kernel,
        out_shape=(shape((2, 256, 1024), bf16), shape((2, 2, 256, 256), bf16)),
        in_specs=[smem, smem, anyspace, anyspace, anyspace, vmem, vmem],
        out_specs=(anyspace, anyspace),
        scratch_shapes=[
            pltpu.VMEM((2, 256, 2048), bf16),
            pltpu.VMEM((2, 256, 2048), bf16),
            pltpu.VMEM((4096, 8, 128), bf16),
            pltpu.VMEM((2048, 8, 128), bf16),
            pltpu.VMEM((4096, 128), f32),
            pltpu.VMEM((4096, 1024), bf16),
            pltpu.VMEM((4096, 512), bf16),
            pltpu.VMEM((2, 256, 1024), f32),
            pltpu.VMEM((2, 256, 512), f32),
            pltpu.VMEM((4, 4, 256, 128), bf16),
            pltpu.VMEM((4, 256, 256), bf16),
            pltpu.VMEM((2, 2, 256, 256), bf16),
            pltpu.VMEM((4, 4, 256, 128), bf16),
            pltpu.VMEM((20, 256, 256), bf16),
            pltpu.VMEM((2, 16, 256), bf16),
            pltpu.VMEM((16, 256), bf16),
            pltpu.VMEM((20, 144, 256), bf16),
            pltpu.VMEM((144, 128), bf16),
            pltpu.VMEM((4, 4, 8, 256), f32),
            pltpu.VMEM((4, 4, 144, 256), f32),
            pltpu.VMEM((4, 4, 256, 256), f32),
            pltpu.VMEM((4, 256, 512), bf16),
            dma(CHUNKS), dma(CHUNKS), dma(3),
            dma(CHUNKS, 3), dma(CHUNKS, 3), dma(CHUNKS),
            dma(CHUNKS, 3), dma(CHUNKS, 3), dma(CHUNKS),
            dma(CHUNKS), dma(CHUNKS), dma(CHUNKS), dma(CHUNKS),
            dma(CHUNKS), dma(CHUNKS), dma(CHUNKS), dma(CHUNKS),
            dma(1), dma(1), dma(1), dma(15), dma(2), dma(1),
            dma(3), dma(3), dma(1),
        ],
        compiler_params=pltpu.CompilerParams(
            collective_id=0, has_side_effects=True, vmem_limit_bytes=VMEM_BYTES
        ),
    )(lengths, sink_positions, prompt_states, q_weight, kv_rows, cos_table, sin_table)
    return attended, cache.reshape(2, 1, 2, 1, 256, 256)


def solution(mesh):
    placed = (
        P(None, ("grp", "seq"), "tp"),
        P(None, "tp", None),
        P(None, None, "tp", None),
        P(),
        P(),
    )
    return jax.shard_map(
        per_device,
        mesh=mesh,
        in_specs=placed,
        out_specs=(P(None, ("grp", "seq"), "tp"), P(None, ("tp", "grp"), None, "seq", None, None)),
        check_vma=False,
    )
```

```python
import math

import jax
import jax.numpy as jnp
from jax import lax
from jax.experimental import pallas as pl
from jax.experimental.pallas import tpu as pltpu
from jax.sharding import PartitionSpec as P

WINDOW = 4096
ROPE_BASE = 10000.0
NEG_FILL = -1e30
FAR = 1 << 30
MESH = pl.DeviceIdType.MESH
CHUNKS = 4
EARLY_SIDE = 2
VMEM_BYTES = 60 * 2**20


def place():
    core, seq, tp = lax.axis_index("grp"), lax.axis_index("seq"), lax.axis_index("tp")
    return core, seq // 8, lax.rem(seq // 4, 2), lax.rem(seq, 4), tp


def at(core, y, x, z, tp):
    return (core, y * 8 + x * 4 + z, tp)


def next_row(core, y):
    wraps = (y + 1) // 4
    return lax.rem(core + wraps, 2), lax.rem(y + 1, 4)


def previous_row(core, y):
    wraps = (4 - y) // 4
    return lax.rem(core + wraps, 2), lax.rem(y + 3, 4)


def remote(src, dst, send_sem, recv_sem, target):
    return pltpu.make_async_remote_copy(
        src_ref=src,
        dst_ref=dst,
        send_sem=send_sem,
        recv_sem=recv_sem,
        device_id=target,
        device_id_type=MESH,
    )


def turned(block, cosine, sine):
    return block * cosine + pltpu.roll(block, 64, 1) * sine


SCALE = math.log2(math.e) / math.sqrt(128.0)


def layer_kernel(
    lens, sinks, x_hbm, wq_hbm, wkv_hbm, cos_ref, sin_ref,
    out_ref, cache_out,
    x_own, x_far, wq_raw, wkv_raw, spread, wq, wkv, acc_q, acc_kv, q_stage, kv_stage, cache_stage,
    q_all, kv_all, sink_all, sink_stage, values, sink_values, peak, total, scores, stage,
    x_send, x_recv, load_sem, kv_send, kv_recv, kv_keep, q_send, q_recv, q_keep,
    a_send, a_recv, b_send, b_recv, aa_send, aa_recv, bb_send, bb_recv,
    c_send, c_recv, c_keep, s_send, s_recv, s_keep, o_send, o_recv, o_keep,
):
    core, y, x, z, tp = place()
    up, down = next_row(core, y), previous_row(core, y)
    ahead, behind = at(*up, x, z, tp), at(*down, x, z, tp)
    partner = at(core, y, x, z, 1 - tp)
    twin = at(1 - core, y, x, z, tp)
    side = at(core, y, 1 - x, z, tp)
    beyond = at(lax.rem(core + (y + 2) // 4, 2), lax.rem(y + 2, 4), x, z, tp)
    before = at(lax.rem(core + (5 - y) // 4, 2), lax.rem(y + 2, 4), x, z, tp)
    first_row = (core + y) == 0
    row = core * 4 + y
    peers = [at(core, y, x, lax.rem(z + d, 4), tp) for d in (1, 2, 3)]

    barrier = pltpu.get_barrier_semaphore()
    for other in [partner, twin, ahead, behind, beyond, before, side, *peers]:
        pl.semaphore_signal(barrier, inc=1, device_id=other, device_id_type=MESH)

    def sink_target(n):
        slot = lax.rem(row * 2 + x + n, 16)
        return at(slot // 8, lax.rem(slot // 2, 4), lax.rem(slot, 2), z, tp)

    @pl.when(first_row)
    def _():
        for n in range(1, 16):
            pl.semaphore_signal(barrier, inc=1, device_id=sink_target(n), device_id_type=MESH)
        pl.semaphore_wait(barrier, 25)

    @pl.when(jnp.logical_not(first_row))
    def _():
        for x_home in (0, 1):
            pl.semaphore_signal(
                barrier, inc=1, device_id=at(0, 0, x_home, z, tp), device_id_type=MESH
            )
        pl.semaphore_wait(barrier, 12)

    request = z // 2
    marks = [sinks[request, n] for n in range(4)]
    fresh = []
    for n in range(4):
        mark = marks[n]
        for earlier in marks[:n]:
            mark = jnp.where(marks[n] == earlier, FAR, mark)
        fresh.append(mark)
    size = 256 // CHUNKS
    spans = [pl.ds(c * size, size) for c in range(CHUNKS)]
    x_copies = [
        remote(x_hbm.at[:, s], x_far.at[:, s], x_send.at[c], x_recv.at[c], partner)
        for c, s in enumerate(spans)
    ]
    for copy in x_copies:
        copy.start()
    load_x = pltpu.make_async_copy(x_hbm, x_own, load_sem.at[0])
    load_kv = pltpu.make_async_copy(wkv_hbm, wkv_raw, load_sem.at[1])
    load_q = pltpu.make_async_copy(wq_hbm, wq_raw, load_sem.at[2])
    load_kv.start()
    load_q.start()
    load_x.start()
    load_kv.wait()

    @pl.loop(0, 4)
    def _(block):
        rows = pl.ds(pl.multiple_of(block * 512, 512), 512)
        spread[...] = wkv_raw[rows].reshape(4096, 128).astype(jnp.float32)
        kept = pl.ds(pl.multiple_of(block * 1024, 1024), 1024)
        for g in range(2):
            for c in range(2):
                at_column = (g * 2 + c) * 128
                wkv[kept, at_column:at_column + 128] = spread[
                    pl.ds(c * 2 + g, 1024, stride=4), :
                ].astype(jnp.bfloat16)

    load_q.wait()

    @pl.loop(0, 8)
    def _(block):
        rows = pl.ds(pl.multiple_of(block * 512, 512), 512)
        spread[...] = wq_raw[rows].reshape(4096, 128).astype(jnp.float32)
        for h in range(8):
            wq[rows, h * 128:(h + 1) * 128] = spread[pl.ds(h, 512, stride=8), :].astype(
                jnp.bfloat16
            )

    load_x.wait()
    own_rows = pl.ds(pl.multiple_of(tp * 2048, 2048), 2048)
    far_rows = pl.ds(pl.multiple_of((1 - tp) * 2048, 2048), 2048)

    def columns(n):
        return pl.ds(pl.multiple_of(n * 256, 256), 256)

    @pl.loop(0, 2)
    def _(n):
        acc_kv[:, :, columns(n)] = jnp.dot(
            x_own[...].reshape(512, 2048),
            wkv[own_rows, columns(n)],
            preferred_element_type=jnp.float32,
        ).reshape(2, 256, 256)

    @pl.loop(0, 4)
    def _(n):
        acc_q[:, :, columns(n)] = jnp.dot(
            x_own[...].reshape(512, 2048),
            wq[own_rows, columns(n)],
            preferred_element_type=jnp.float32,
        ).reshape(2, 256, 256)

    slab_start = (core * 32 + y * 8 + x * 4 + z) * 256
    pending = []
    kv_copies, q_copies, keeps, a_copies, b_copies, aa_copies = [], [], [], [], [], []

    side_source = pl.ds(16 - 8 * x, 4)

    def to_side(c):
        s = spans[c]
        a_copies[c].wait_recv()
        b = remote(
            kv_all.at[side_source, s], kv_all.at[12:16, s], b_send.at[c], b_recv.at[c], side
        )
        b.start()
        b_copies.append(b)

    def from_side(c):
        s = pl.ds(pl.multiple_of(c * size, size), size)
        remote(
            kv_all.at[side_source, s], kv_all.at[12:16, s], b_send.at[c], b_recv.at[c], side
        ).wait_recv()
        remote(
            kv_all.at[12:16, s], kv_all.at[4:8, s], bb_send.at[c], bb_recv.at[c], ahead
        ).start()

    for c in range(CHUNKS):
        s = spans[c]
        x_copies[c].wait_recv()
        if c == 2:
            for early in range(EARLY_SIDE):
                to_side(early)
        if c == CHUNKS - 1:
            for late in range(EARLY_SIDE, CHUNKS - 1):
                to_side(late)
        cosine, sine = cos_ref[s, :], sin_ref[s, :]

        @pl.loop(0, 2)
        def _(n):
            total = jnp.dot(
                x_far[:, s].reshape(2 * size, 2048),
                wkv[far_rows, columns(n)],
                preferred_element_type=jnp.float32,
            )
            for r in range(2):
                block = total[r * size:(r + 1) * size] + acc_kv[r, s, columns(n)]
                keys = turned(block[:, :128], cosine, sine).astype(jnp.bfloat16)
                both = jnp.concatenate([keys, block[:, 128:].astype(jnp.bfloat16)], axis=1)
                kv_stage[r * 2 + n, s, :] = both
                position = (
                    slab_start + c * size + lax.broadcasted_iota(jnp.int32, (size, 256), 0)
                )
                cache_stage[r, n, s, :] = jnp.where(
                    position < lens[r], both.astype(jnp.float32), 0.0
                ).astype(jnp.bfloat16)

        for d in (1, 2, 3):
            target = lax.rem(z + d, 4)
            copy = remote(
                kv_stage.at[target, s], kv_all.at[16 + z, s],
                kv_send.at[c, d - 1], kv_recv.at[c, d - 1], peers[d - 1],
            )
            copy.start()
            kv_copies.append(copy)
        keep = pltpu.make_async_copy(kv_stage.at[z, s], kv_all.at[16 + z, s], kv_keep.at[c])
        keep.start()

        @pl.loop(0, 4)
        def _(n):
            total = jnp.dot(
                x_far[:, s].reshape(2 * size, 2048),
                wq[far_rows, columns(n)],
                preferred_element_type=jnp.float32,
            )
            for r in range(2):
                block = total[r * size:(r + 1) * size] + acc_q[r, s, columns(n)]
                for k in range(2):
                    head = turned(block[:, k * 128:(k + 1) * 128], cosine, sine)
                    q_stage[r * 2 + n // 2, lax.rem(n, 2) * 2 + k, s, :] = head.astype(
                        jnp.bfloat16
                    )

        for d in (1, 2, 3):
            target = lax.rem(z + d, 4)
            copy = remote(
                q_stage.at[target, :, s], q_all.at[z, :, s],
                q_send.at[c, d - 1], q_recv.at[c, d - 1], peers[d - 1],
            )
            copy.start()
            q_copies.append(copy)
        q_own = pltpu.make_async_copy(q_stage.at[z, :, s], q_all.at[z, :, s], q_keep.at[c])
        q_own.start()
        keeps.append(q_own)

        keep.wait()
        for d in range(3):
            kv_copies[c * 3 + d].wait_recv()
        a = remote(kv_all.at[16:20, s], kv_all.at[8:12, s], a_send.at[c], a_recv.at[c], ahead)
        a.start()
        a_copies.append(a)
        aa = remote(kv_all.at[16:20, s], kv_all.at[0:4, s], aa_send.at[c], aa_recv.at[c], beyond)
        aa.start()
        aa_copies.append(aa)
        if c == CHUNKS - 1:
            for early in range(EARLY_SIDE):
                from_side(early)

    cache_copy = remote(
        cache_stage.at[:, 1 - core], cache_out.at[:, core], c_send.at[0], c_recv.at[0], twin
    )
    cache_copy.start()
    cache_keep = pltpu.make_async_copy(
        cache_stage.at[:, core], cache_out.at[:, core], c_keep.at[0]
    )
    cache_keep.start()

    sink_sends = [
        remote(
            sink_stage, sink_all.at[x], s_send.at[n - 1], s_recv.at[x], sink_target(n)
        )
        for n in range(1, 16)
    ]
    sink_keep = pltpu.make_async_copy(sink_stage, sink_all.at[x], s_keep.at[0])

    @pl.when(first_row)
    def _():
        mark_row = lax.broadcasted_iota(jnp.int32, (16, 1024), 0)
        token = row * 2048 + x * 1024 + lax.broadcasted_iota(jnp.int32, (16, 1024), 1)
        wanted = jnp.full((16, 1024), FAR, jnp.int32)
        for n in range(4):
            wanted = jnp.where(mark_row == n, marks[n], wanted)
        hot = jnp.where(token == wanted, 1.0, 0.0).astype(jnp.bfloat16)
        sink_stage[...] = jnp.dot(
            hot, kv_all[16:20].reshape(1024, 256), preferred_element_type=jnp.float32
        ).astype(jnp.bfloat16)
        for copy in sink_sends:
            copy.start()
        sink_keep.start()

    to_side(CHUNKS - 1)
    for copy in keeps:
        copy.wait()
    for copy in q_copies:
        copy.wait_recv()
    group = row * 2 + x
    length = lens[request]
    key_at = lax.broadcasted_iota(jnp.int32, (256, 256), 0)
    query_at = lax.broadcasted_iota(jnp.int32, (256, 256), 1)

    def turn_values(first, count):
        @pl.loop(first, first + count)
        def _(slab):
            values[slab, :128, :] = (
                kv_all[slab, :, 128:].astype(jnp.float32).T.astype(jnp.bfloat16)
            )
            values[slab, 128:, :] = jnp.ones((16, 256), jnp.bfloat16)

    def rescale(j, h, new, gained):
        factor = jnp.exp2((peak[j, h] - new) * SCALE)
        peak[j, h] = new
        total[j, h] = (total[j, h].reshape(18, 8, 256) * factor[None]).reshape(144, 256) + gained

    def top_of(block):
        return jnp.broadcast_to(jnp.max(block, axis=0, keepdims=True), (8, 256))

    def fold(j, items):
        tops = []
        for h in range(4):
            top = peak[j, h]
            for i, (slab, visible) in enumerate(items):
                block = lax.dot_general(
                    kv_all[slab, :, :128], q_all[j, h], (((1,), (1,)), ((), ())),
                    preferred_element_type=jnp.float32,
                )
                if visible is not None:
                    block = jnp.where(visible, block, NEG_FILL)
                scores[h, i] = block
                top = jnp.maximum(top, jnp.max(block.reshape(32, 8, 256), axis=0))
            tops.append(top_of(top))
        for h in range(4):
            shift = tops[h] * SCALE
            gained = None
            for i, (slab, _) in enumerate(items):
                weights = jnp.exp2(
                    (scores[h, i] * SCALE).reshape(32, 8, 256) - shift[None]
                ).reshape(256, 256)
                part = jnp.dot(
                    values[slab], weights.astype(jnp.bfloat16),
                    preferred_element_type=jnp.float32,
                )
                gained = part if gained is None else gained + part
            rescale(j, h, tops[h], gained)

    turn_values(16, 4)

    @pl.loop(0, 4)
    def _(j):
        for h in range(4):
            peak[j, h] = jnp.full((8, 256), NEG_FILL, jnp.float32)
            total[j, h] = jnp.zeros((144, 256), jnp.float32)
        fold(j, [(16 + j, key_at <= query_at)])

    turn_values(8, 4)

    @pl.when(group >= 2)
    def _():
        @pl.loop(0, 4)
        def _(j):
            fold(j, [(8 + i, None) for i in range(4)])

    for copy in aa_copies:
        copy.wait_recv()
    turn_values(0, 4)

    @pl.loop(0, CHUNKS)
    def _(j):
        @pl.when(j < CHUNKS - EARLY_SIDE)
        def _():
            from_side(j + EARLY_SIDE)

        @pl.when(group >= 4)
        def _():
            edges = [(jnp.where(t < j, 16 + t, t + 1), None) for t in range(3)]
            fold(j, edges + [(j, key_at > query_at)])

        @pl.when(group < 4)
        def _():
            def inner(t, carry):
                fold(j, [(16 + t, None)])
                return carry

            lax.fori_loop(0, j, inner, 0)

    turn_values(12, 4)

    @pl.when(group >= 1)
    def _():
        @pl.loop(0, 4)
        def _(j):
            fold(j, [(12 + i, None) for i in range(4)])

    bb_copies = [
        remote(kv_all.at[12:16, s], kv_all.at[4:8, s], bb_send.at[c], bb_recv.at[c], ahead)
        for c, s in enumerate(spans)
    ]
    for copy in bb_copies:
        copy.wait_recv()
    turn_values(4, 4)
    @pl.when(first_row)
    def _():
        sink_keep.wait()
        for copy in sink_sends:
            copy.wait_send()
        remote(sink_stage, sink_all.at[1 - x], s_send.at[0], s_recv.at[1 - x], partner).wait_recv()

    @pl.when(jnp.logical_not(first_row))
    def _():
        for home in (0, 1):
            remote(
                sink_stage, sink_all.at[home], s_send.at[0], s_recv.at[home], partner
            ).wait_recv()
    sink_kv = (sink_all[0].astype(jnp.float32) + sink_all[1].astype(jnp.float32)).astype(
        jnp.bfloat16
    )
    sink_values[:128, :] = (
        jnp.concatenate(
            [sink_kv[:, 128:].astype(jnp.float32), jnp.zeros((112, 128), jnp.float32)], axis=0
        ).T.astype(jnp.bfloat16)
    )
    sink_values[128:, :] = jnp.ones((16, 128), jnp.bfloat16)
    mark_at = lax.broadcasted_iota(jnp.int32, (16, 256), 0)
    sink_at = jnp.full((16, 256), FAR, jnp.int32)
    for n in range(4):
        sink_at = jnp.where(mark_at == n, fresh[n], sink_at)
    out_columns = pl.ds(pl.multiple_of(lax.rem(z, 2) * 512, 512), 512)

    @pl.loop(0, 4)
    def _(turn):
        j = lax.rem(z + 1 + turn, 4)

        @pl.when(group >= 3)
        def _():
            fold(j, [(4 + i, None) for i in range(4)])

        first = (group * 4 + j) * 256
        far = first + query_at[:16] - sink_at >= WINDOW
        for h in range(4):
            block = lax.dot_general(
                sink_kv[:, :128], q_all[j, h], (((1,), (1,)), ((), ())),
                preferred_element_type=jnp.float32,
            )
            block = jnp.where(far, block, NEG_FILL)
            top = top_of(
                jnp.maximum(peak[j, h], jnp.max(block.reshape(2, 8, 256), axis=0))
            )
            weights = jnp.exp2((block * SCALE).reshape(2, 8, 256) - (top * SCALE)[None])
            weights = jnp.concatenate(
                [weights.reshape(16, 256), jnp.zeros((112, 256), jnp.float32)], axis=0
            )
            rescale(
                j, h, top,
                jnp.dot(
                    sink_values[...], weights.astype(jnp.bfloat16),
                    preferred_element_type=jnp.float32,
                ),
            )
            mixed = (total[j, h, :128] / total[j, h, 128:129]).T
            live = first + lax.broadcasted_iota(jnp.int32, (256, 128), 0) < length
            stage[turn, :, h * 128:(h + 1) * 128] = jnp.where(live, mixed, 0.0).astype(
                jnp.bfloat16
            )

        home = out_ref.at[request, :, out_columns]

        @pl.when(turn < 3)
        def _():
            remote(
                stage.at[turn], home, o_send.at[turn], o_recv.at[turn],
                at(core, y, x, j, tp),
            ).start()

        @pl.when(turn == 3)
        def _():
            pltpu.make_async_copy(stage.at[turn], home, o_keep.at[0]).start()

    pltpu.make_async_copy(
        stage.at[3], out_ref.at[request, :, out_columns], o_keep.at[0]
    ).wait()
    for turn in range(3):
        source = lax.rem(z + 3 - turn, 4)
        landed = out_ref.at[
            source // 2, :, pl.ds(pl.multiple_of(lax.rem(source, 2) * 512, 512), 512)
        ]
        remote(
            stage.at[turn], landed, o_send.at[turn], o_recv.at[turn], peers[turn]
        ).wait()
    cache_keep.wait()
    cache_copy.wait()
    for copy in aa_copies + bb_copies + q_copies + kv_copies + a_copies + b_copies + x_copies:
        copy.wait_send()


def dma(*shape):
    return pltpu.SemaphoreType.DMA(shape)


def per_device(prompt_states, q_weight, kv_weight, lengths, sink_positions):
    bf16 = jnp.bfloat16
    core, y, x, z, tp = place()
    group = (core * 4 + y) * 2 + x
    kv_rows = kv_weight.reshape(2048, 8, 128)
    positions = (group * 4 + z) * 256 + jnp.arange(256, dtype=jnp.int32)
    ladder = jnp.arange(64, dtype=jnp.float32) * (2.0 / 128)
    inv_freq = jnp.exp(-math.log(ROPE_BASE) * ladder)
    angles = positions.astype(jnp.float32)[:, None] * inv_freq[None, :]
    cosine, sine = jnp.cos(angles), jnp.sin(angles)
    cos_table = jnp.concatenate([cosine, cosine], axis=1)
    sin_table = jnp.concatenate([-sine, sine], axis=1)
    anyspace = pl.BlockSpec(memory_space=pl.ANY)
    vmem = pl.BlockSpec(memory_space=pltpu.VMEM)
    smem = pl.BlockSpec(memory_space=pltpu.SMEM)
    shape = jax.ShapeDtypeStruct
    f32 = jnp.float32
    attended, cache = pl.pallas_call(
        layer_kernel,
        out_shape=(shape((2, 256, 1024), bf16), shape((2, 2, 256, 256), bf16)),
        in_specs=[smem, smem, anyspace, anyspace, anyspace, vmem, vmem],
        out_specs=(anyspace, anyspace),
        scratch_shapes=[
            pltpu.VMEM((2, 256, 2048), bf16),
            pltpu.VMEM((2, 256, 2048), bf16),
            pltpu.VMEM((4096, 8, 128), bf16),
            pltpu.VMEM((2048, 8, 128), bf16),
            pltpu.VMEM((4096, 128), f32),
            pltpu.VMEM((4096, 1024), bf16),
            pltpu.VMEM((4096, 512), bf16),
            pltpu.VMEM((2, 256, 1024), f32),
            pltpu.VMEM((2, 256, 512), f32),
            pltpu.VMEM((4, 4, 256, 128), bf16),
            pltpu.VMEM((4, 256, 256), bf16),
            pltpu.VMEM((2, 2, 256, 256), bf16),
            pltpu.VMEM((4, 4, 256, 128), bf16),
            pltpu.VMEM((20, 256, 256), bf16),
            pltpu.VMEM((2, 16, 256), bf16),
            pltpu.VMEM((16, 256), bf16),
            pltpu.VMEM((20, 144, 256), bf16),
            pltpu.VMEM((144, 128), bf16),
            pltpu.VMEM((4, 4, 8, 256), f32),
            pltpu.VMEM((4, 4, 144, 256), f32),
            pltpu.VMEM((4, 4, 256, 256), f32),
            pltpu.VMEM((4, 256, 512), bf16),
            dma(CHUNKS), dma(CHUNKS), dma(3),
            dma(CHUNKS, 3), dma(CHUNKS, 3), dma(CHUNKS),
            dma(CHUNKS, 3), dma(CHUNKS, 3), dma(CHUNKS),
            dma(CHUNKS), dma(CHUNKS), dma(CHUNKS), dma(CHUNKS),
            dma(CHUNKS), dma(CHUNKS), dma(CHUNKS), dma(CHUNKS),
            dma(1), dma(1), dma(1), dma(15), dma(2), dma(1),
            dma(3), dma(3), dma(1),
        ],
        compiler_params=pltpu.CompilerParams(
            collective_id=0, has_side_effects=True, vmem_limit_bytes=VMEM_BYTES
        ),
    )(lengths, sink_positions, prompt_states, q_weight, kv_rows, cos_table, sin_table)
    return attended, cache.reshape(2, 1, 2, 1, 256, 256)


def solution(mesh):
    placed = (
        P(None, ("grp", "seq"), "tp"),
        P(None, "tp", None),
        P(None, None, "tp", None),
        P(),
        P(),
    )
    return jax.shard_map(
        per_device,
        mesh=mesh,
        in_specs=placed,
        out_specs=(P(None, ("grp", "seq"), "tp"), P(None, ("tp", "grp"), None, "seq", None, None)),
        check_vma=False,
    )
```
